64 devices in a mesh: data: 4 (over x, y), sp: 16 (over z, core).
Axes of the slice: x: 2, y: 2, z: 8, core: 2. Of those that a mesh axis runs over, the one named last changes fastest.
The devices are a block of a 4x4x8 slice.
Arguments:
- latent: bfloat16 [4, 96, 768, 1152], P('data', 'sp'), parts along dimension 0
- ln_gain: bfloat16 [4, 1152], replicated
- ln_bias: bfloat16 [4, 1152], replicated
- w_qkv: bfloat16 [2, 1152, 3, 16, 72], replicated
- w_out: bfloat16 [2, 16, 72, 1152], replicated
- w_up: bfloat16 [2, 1152, 4608], replicated
- w_down: bfloat16 [2, 4608, 1152], replicated
Outputs:
- output: bfloat16 [4, 96, 768, 1152], P('data', 'sp'), parts along dimension 0
There are 4 independent parts. The reference program is written for one: setup_inputs(seed, part) draws one part's arguments, and reference() takes and returns one part's arrays. A program takes and returns all parts, laid end to end along the dimension named above; an argument that names none is the same for every part.
All inputs are finite; a program needn't handle non-finite values.
Results may differ from the reference program's by a relative error of at most 0.0125955.
Values are sent between devices in bfloat16 or wider.
A program may use at most 768 MiB of HBM per device.

```python
import jax
import jax.numpy as jnp
from jax import lax
from functools import partial

FRAMES = 96
PATCHES = 768
WIDTH = 1152
NUM_HEADS = 16
HEAD_DIM = WIDTH // NUM_HEADS
LN_EPS = 1e-6


def setup_inputs(seed: int = 0, part: int = 0) -> dict:
    part_key = jax.random.fold_in(jax.random.key(seed), part)
    noise_key, frame_key, patch_key = jax.random.split(part_key, 3)
    noise = jax.random.normal(noise_key, (1, FRAMES, PATCHES, WIDTH), jnp.float32)
    frame_sig = jax.random.normal(frame_key, (1, FRAMES, 1, WIDTH), jnp.float32)
    patch_sig = jax.random.normal(patch_key, (1, 1, PATCHES, WIDTH), jnp.float32)
    latent = 0.6 * noise + frame_sig + 0.8 * patch_sig
    weight_keys = jax.random.split(jax.random.key(seed + 1), 6)
    qk_boost = jnp.array([1.3, 1.3, 1.0], jnp.float32).reshape(1, 1, 3, 1, 1)
    ln_gain = 1.0 + 0.4 * jax.random.normal(weight_keys[0], (4, WIDTH), jnp.float32)
    ln_bias = 0.5 * jax.random.normal(weight_keys[1], (4, WIDTH), jnp.float32)
    w_qkv = jax.random.normal(weight_keys[2], (2, WIDTH, 3, NUM_HEADS, HEAD_DIM), jnp.float32) * qk_boost * WIDTH ** -0.5
    w_out = jax.random.normal(weight_keys[3], (2, NUM_HEADS, HEAD_DIM, WIDTH), jnp.float32) * WIDTH ** -0.5
    w_up = jax.random.normal(weight_keys[4], (2, WIDTH, 4 * WIDTH), jnp.float32) * WIDTH ** -0.5
    w_down = jax.random.normal(weight_keys[5], (2, 4 * WIDTH, WIDTH), jnp.float32) * (4 * WIDTH) ** -0.5
    return {
        'latent': latent.astype(jnp.bfloat16),
        'ln_gain': ln_gain.astype(jnp.bfloat16),
        'ln_bias': ln_bias.astype(jnp.bfloat16),
        'w_qkv': w_qkv.astype(jnp.bfloat16),
        'w_out': w_out.astype(jnp.bfloat16),
        'w_up': w_up.astype(jnp.bfloat16),
        'w_down': w_down.astype(jnp.bfloat16),
    }


def layer_norm(tokens, gain_vec, shift_vec):
    as_float = tokens.astype(jnp.float32)
    mean_val = jnp.mean(as_float, axis=-1, keepdims=True)
    centered = as_float - mean_val
    variance = jnp.mean(centered * centered, axis=-1, keepdims=True)
    normed = centered * lax.rsqrt(variance + LN_EPS) * gain_vec.astype(jnp.float32) + shift_vec.astype(jnp.float32)
    return normed.astype(jnp.bfloat16)


def seq_block(sequence, layer_idx, ln_gain, ln_bias, w_qkv, w_out, w_up, w_down):
    length = sequence.shape[0]
    normed = layer_norm(sequence, ln_gain[2 * layer_idx], ln_bias[2 * layer_idx])
    qkv_all = jnp.dot(normed, w_qkv[layer_idx].reshape(WIDTH, 3 * WIDTH), preferred_element_type=jnp.float32).astype(jnp.bfloat16)
    qkv_all = qkv_all.reshape(length, 3, NUM_HEADS, HEAD_DIM).astype(jnp.float32)
    scores = jnp.einsum('qhk,phk->hqp', qkv_all[:, 0], qkv_all[:, 1]) * HEAD_DIM ** -0.5
    attn_probs = jax.nn.softmax(scores, axis=-1).astype(jnp.bfloat16)
    attended = jnp.einsum('hqp,phk->qhk', attn_probs.astype(jnp.float32), qkv_all[:, 2]).astype(jnp.bfloat16)
    projected = jnp.dot(attended.reshape(length, WIDTH), w_out[layer_idx].reshape(WIDTH, WIDTH), preferred_element_type=jnp.float32)
    residual = (sequence.astype(jnp.float32) + projected).astype(jnp.bfloat16)
    normed_mlp = layer_norm(residual, ln_gain[2 * layer_idx + 1], ln_bias[2 * layer_idx + 1])
    hidden = jax.nn.gelu(jnp.dot(normed_mlp, w_up[layer_idx], preferred_element_type=jnp.float32), approximate=True).astype(jnp.bfloat16)
    result = residual.astype(jnp.float32) + jnp.dot(hidden, w_down[layer_idx], preferred_element_type=jnp.float32)
    return result.astype(jnp.bfloat16)


def reference(latent, ln_gain, ln_bias, w_qkv, w_out, w_up, w_down):
    space_fn = partial(seq_block, layer_idx=0, ln_gain=ln_gain, ln_bias=ln_bias, w_qkv=w_qkv, w_out=w_out, w_up=w_up, w_down=w_down)
    spatial = lax.map(space_fn, latent[0])
    time_fn = partial(seq_block, layer_idx=1, ln_gain=ln_gain, ln_bias=ln_bias, w_qkv=w_qkv, w_out=w_out, w_up=w_up, w_down=w_down)
    temporal = lax.map(time_fn, jnp.swapaxes(spatial, 0, 1))
    return jnp.swapaxes(temporal, 0, 1)[None]
```

```python
import functools

import jax
import jax.numpy as jnp
from jax import lax
from jax.experimental import pallas as pl
from jax.experimental.pallas import tpu as pltpu
from jax.sharding import PartitionSpec as P

F32 = jnp.float32
BF16 = jnp.bfloat16
MESH = pl.DeviceIdType.MESH
LN_EPS = 1e-6
LOG2E = 1.4426950408889634
GROUP = 16
LANES = 8
QB = 256
KB = 128
RB = 32
UPB = 512
SLOTS = 3


def normalize(rows, gain, shift):
    inv = 1.0 / rows.shape[-1]
    cent = rows - jnp.sum(rows, axis=-1, keepdims=True) * inv
    var = jnp.sum(cent * cent, axis=-1, keepdims=True) * inv
    return (cent * lax.rsqrt(var + LN_EPS) * gain + shift).astype(BF16)


def gelu(x):
    c = 0.7978845608028654
    half = 0.5 * x
    return half + half * jnp.tanh(x * (c + (c * 0.044715) * (x * x)))


def fold(t, op):
    acc = t[0:8]
    for r in range(8, t.shape[0], 8):
        acc = op(acc, t[r:r + 8])
    return acc


def aligned(i, step):
    return pl.ds(pl.multiple_of(i * step, step), step)


def block_kernel(cfg, x_hbm, gain_ref, bias_ref, wqkv_hbm, wout_hbm, wup_hbm, wdown_hbm, y_hbm,
                 wqkv, wout, wup, wdown, xin, a, qkvt, ot, h, nb, u, y, s0, s1, p0, p1, m0, m1, l0, l1,
                 wsem, xsem, send_sem, recv_sem, own_sem):
    layer, temporal, n, units, tok, heads, hd = cfg
    width = heads * hd
    ff = wup.shape[1]
    per = tok // n
    tiles = per // GROUP
    rows = n * GROUP
    sbuf, pbuf, mbuf, lbuf = (s0, s1), (p0, p1), (m0, m1), (l0, l1)
    cscale = (hd ** -0.5) * LOG2E
    me = lax.axis_index('sp')

    def xcopy(unit, slot):
        src = x_hbm.at[:, aligned(unit, LANES), :] if temporal else x_hbm.at[unit]
        return pltpu.make_async_copy(src, xin.at[slot], xsem.at[slot])

    wcopies = [pltpu.make_async_copy(src.at[layer], dst, wsem.at[i]) for i, (src, dst) in enumerate(
        ((wqkv_hbm, wqkv), (wout_hbm, wout), (wup_hbm, wup), (wdown_hbm, wdown)))]
    xcopy(0, 0).start()
    for c in wcopies:
        c.start()

    barrier = pltpu.get_barrier_semaphore()
    for k in range(1, n):
        pl.semaphore_signal(barrier, inc=1, device_id={'sp': lax.rem(me + k, n)}, device_id_type=MESH)

    def target(unit, t):
        if temporal:
            return y_hbm.at[pl.ds(2 * t, 2), pl.ds(pl.multiple_of(me * (units * LANES) + unit * LANES, LANES), LANES), :]
        return y_hbm.at[me * units + unit, aligned(t, GROUP), :]

    def send(unit, t, slot, k):
        d = lax.rem(me + k, n)
        return pltpu.make_async_remote_copy(
            src_ref=y.at[slot, d], dst_ref=target(unit, t), send_sem=send_sem.at[slot], recv_sem=recv_sem,
            device_id={'sp': d}, device_id_type=MESH)

    def keep(unit, t, slot):
        return pltpu.make_async_copy(y.at[slot, me], target(unit, t), own_sem.at[slot])

    def drain(slot):
        keep(0, 0, slot).wait()
        whole = y.at[slot, pl.ds(0, n - 1)]
        pltpu.make_async_copy(whole, whole, send_sem.at[slot]).wait()

    def load_x(slot, block):
        if temporal:
            return xin[slot, aligned(block, QB // LANES)].reshape(QB, width).astype(F32)
        return xin[slot, aligned(block, QB), :].astype(F32)

    gains = [gain_ref[2 * layer + i:2 * layer + i + 1, :].astype(F32) for i in range(2)]
    shifts = [bias_ref[2 * layer + i:2 * layer + i + 1, :].astype(F32) for i in range(2)]

    def pre_norm(slot, block):
        a[aligned(block, QB), :] = normalize(load_x(slot, block), gains[0], shifts[0])

    nq, nk = tok // QB, tok // KB
    cols = [slice(b * QB, (b + 1) * QB) for b in range(nq)]

    def score(hh, par, c):
        k = qkvt[heads + hh, :, c * KB:(c + 1) * KB]
        for b in range(nq):
            s = lax.dot_general(k, qkvt[hh, :, cols[b]], (((0,), (0,)), ((), ())), preferred_element_type=F32)
            if temporal:
                row = lax.broadcasted_iota(jnp.int32, s.shape, 0)
                col = lax.broadcasted_iota(jnp.int32, s.shape, 1)
                s = jnp.where((row & (LANES - 1)) == (col & (LANES - 1)), s, -1e38)
            sbuf[par][c * KB:(c + 1) * KB, cols[b]] = s
            yield fold(s, jnp.maximum)

    def soften(par, ms, c):
        for b in range(nq):
            l = None
            for r in range(c * KB, (c + 1) * KB, RB):
                e = jnp.exp2((sbuf[par][r:r + RB, cols[b]] - ms[b]) * cscale)
                pbuf[par][r:r + RB, cols[b]] = e.astype(BF16)
                f = fold(e, jnp.add)
                l = f if l is None else l + f
            yield l

    def mix(hh, par, b):
        o = jnp.dot(qkvt[2 * heads + hh], pbuf[par][:, cols[b]], preferred_element_type=F32)
        ot[pl.ds(pl.multiple_of(hh * hd, 8), hd), cols[b]] = o * lbuf[par][:, cols[b]]

    def attend(hs, hm, j):
        ms = [jnp.max(mbuf[j][:, cl], axis=0, keepdims=True) for cl in cols]
        mx = ls = None
        for c in range(nk):
            fm, fl = [], []
            for x, z in zip(score(hs, 1 - j, c), soften(j, ms, c)):
                fm.append(x)
                fl.append(z)
            mx = fm if mx is None else [jnp.maximum(p, q) for p, q in zip(mx, fm)]
            ls = fl if ls is None else [p + q for p, q in zip(ls, fl)]
            if (c + 1) % (nk // nq) == 0:
                mix(hm, 1 - j, (c + 1) // (nk // nq) - 1)
        for b in range(nq):
            mbuf[1 - j][:, cols[b]] = mx[b]
            lbuf[j][:, cols[b]] = 1.0 / jnp.sum(ls[b], axis=0, keepdims=True)

    def unit_body(unit, _):
        slot = lax.rem(unit, 2)

        @pl.when(unit == 0)
        def _():
            xcopy(0, 0).wait()
            for b in range(nq):
                pre_norm(0, b)
            wcopies[0].wait()

        @pl.when(unit + 1 < units)
        def _():
            xcopy(unit + 1, 1 - slot).start()

        def qkv_body(i, _):
            r = lax.dot_general(wqkv[aligned(i, width), :], a[...], (((1,), (1,)), ((), ())), preferred_element_type=F32)
            qkvt[pl.ds(heads * i, heads)] = r.reshape(heads, hd, tok).astype(BF16)
            return 0
        lax.fori_loop(0, 3, qkv_body, 0)

        first = None
        for c in range(nk):
            fm = list(score(0, 0, c))
            first = fm if first is None else [jnp.maximum(p, q) for p, q in zip(first, fm)]
        for b in range(nq):
            mbuf[0][:, cols[b]] = first[b]

        def attn_body(i, _):
            def part(j):
                hh = 2 * i + j
                attend(jnp.minimum(hh + 1, heads - 1), jnp.maximum(hh - 1, 0), j)
            part(0)

            @pl.when(i < heads)
            def _():
                part(1)
            return 0
        lax.fori_loop(0, heads // 2, attn_body, 0)

        @pl.when(unit == 0)
        def _():
            wcopies[1].wait()

        for b in range(nq):
            mix(heads - 1, 1, b)
            p = lax.dot_general(ot[:, cols[b]].astype(BF16), wout[...], (((0,), (0,)), ((), ())),
                                preferred_element_type=F32)
            hv = (load_x(slot, b) + p).astype(BF16)
            g = QB // GROUP
            h[b * g:(b + 1) * g] = hv.reshape(g, GROUP, width)
            nb[b * g:(b + 1) * g] = normalize(hv.astype(F32), gains[1], shifts[1]).reshape(g, GROUP, width)

        @pl.when(unit == 0)
        def _():
            wcopies[2].wait()
            wcopies[3].wait()
            pl.semaphore_wait(barrier, n - 1)

        @pl.when(unit + 1 < units)
        def _():
            xcopy(unit + 1, 1 - slot).wait()

        def mlp_body(t, _):
            step = unit * tiles + t
            ys = lax.rem(step, SLOTS)

            @pl.when(step >= SLOTS)
            def _():
                drain(ys)
            hb = jnp.concatenate([h[d * tiles + t] for d in range(n)])
            nbt = jnp.concatenate([nb[d * tiles + t] for d in range(n)])
            for c in range(0, ff, UPB):
                u[:, c:c + UPB] = gelu(jnp.dot(nbt, wup[:, c:c + UPB], preferred_element_type=F32)).astype(BF16)
            cut = ff - UPB
            r = jnp.dot(u[:, :cut], wdown[:cut, :], preferred_element_type=F32)
            r = r + jnp.dot(u[:, cut:], wdown[cut:, :], preferred_element_type=F32)
            y[ys] = (hb.astype(F32) + r).astype(BF16).reshape(y.shape[1:])
            pre_norm(1 - slot, t)
            for k in range(1, n):
                send(unit, t, ys, k).start()
            keep(unit, t, ys).start()
            return 0
        lax.fori_loop(0, tiles, mlp_body, 0)
        return 0

    lax.fori_loop(0, units, unit_body, 0)
    for s in range(SLOTS):
        drain(s)
    if temporal:
        got = y_hbm.at[:, pl.ds(0, (n - 1) * units * LANES), :]
    else:
        got = y_hbm.at[pl.ds(0, (n - 1) * units)]
    pltpu.make_async_copy(got, got, recv_sem).wait()


def run_block(layer, temporal, n, heads, hd, x, gain, bias, wqkv, wout, wup, wdown):
    width = heads * hd
    ff = wup.shape[-1]
    if temporal:
        frames, per, _ = x.shape
        units, tok = per // LANES, frames * LANES
        out = jax.ShapeDtypeStruct((frames // n, per * n, width), BF16)
        xs, ys = (2, frames, LANES, width), (SLOTS, n, GROUP // LANES, LANES, width)
    else:
        units, tok, _ = x.shape
        out = jax.ShapeDtypeStruct((units * n, tok // n, width), BF16)
        xs, ys = (2, tok, width), (SLOTS, n, GROUP, width)
    anyspec = pl.BlockSpec(memory_space=pl.ANY)
    vspec = pl.BlockSpec(memory_space=pltpu.VMEM)
    sent = units * tok * width * 2
    return pl.pallas_call(
        functools.partial(block_kernel, (layer, temporal, n, units, tok, heads, hd)),
        out_shape=out,
        in_specs=[anyspec, vspec, vspec] + [anyspec] * 4,
        out_specs=anyspec,
        scratch_shapes=[
            pltpu.VMEM((3 * width, width), BF16), pltpu.VMEM((width, width), BF16),
            pltpu.VMEM((width, ff), BF16), pltpu.VMEM((ff, width), BF16),
            pltpu.VMEM(xs, BF16), pltpu.VMEM((tok, width), BF16),
            pltpu.VMEM((3 * heads, hd, tok), BF16), pltpu.VMEM((width, tok), F32),
            pltpu.VMEM((tok // GROUP, GROUP, width), BF16), pltpu.VMEM((tok // GROUP, GROUP, width), BF16),
            pltpu.VMEM((n * GROUP, ff), BF16), pltpu.VMEM(ys, BF16),
            pltpu.VMEM((tok, tok), F32), pltpu.VMEM((tok, tok), F32),
            pltpu.VMEM((tok, tok), BF16), pltpu.VMEM((tok, tok), BF16),
            pltpu.VMEM((8, tok), F32), pltpu.VMEM((8, tok), F32),
            pltpu.VMEM((1, tok), F32), pltpu.VMEM((1, tok), F32),
            pltpu.SemaphoreType.DMA((4,)), pltpu.SemaphoreType.DMA((2,)), pltpu.SemaphoreType.DMA((SLOTS,)),
            pltpu.SemaphoreType.DMA, pltpu.SemaphoreType.DMA((SLOTS,)),
        ],
        compiler_params=pltpu.CompilerParams(
            vmem_limit_bytes=67043328, collective_id=layer, has_side_effects=True),
        cost_estimate=pl.CostEstimate(flops=24 * units * tok * width * width, bytes_accessed=3 * sent, transcendentals=0),
        name=f'block{layer}',
    )(x, gain, bias, wqkv, wout, wup, wdown)


def solution(mesh):
    act_spec = P('data', 'sp', None, None)
    n = mesh.shape['sp']

    def local_run(x, gain, bias, w_qkv, w_out, w_up, w_down):
        layers, width, _, heads, hd = w_qkv.shape
        wqkvt = jnp.transpose(w_qkv, (0, 2, 3, 4, 1)).reshape(layers, 3 * width, width)
        wo = w_out.reshape(layers, width, width)
        y = run_block(0, False, n, heads, hd, x[0], gain, bias, wqkvt, wo, w_up, w_down)
        y = run_block(1, True, n, heads, hd, y, gain, bias, wqkvt, wo, w_up, w_down)
        return y[None]

    return jax.shard_map(local_run, mesh=mesh, in_specs=(act_spec,) + (P(),) * 6, out_specs=act_spec, check_vma=False)
```

```python
import functools

import jax
import jax.numpy as jnp
from jax import lax
from jax.experimental import pallas as pl
from jax.experimental.pallas import tpu as pltpu
from jax.sharding import PartitionSpec as P

F32 = jnp.float32
BF16 = jnp.bfloat16
MESH = pl.DeviceIdType.MESH
LN_EPS = 1e-6
LOG2E = 1.4426950408889634
SUB = 8
PAIR = 2
LANE = 128
QB = 256
KB = 128
RB = 32
UPB = 512
SLOTS = 3
NEG = -1e38


def normalize(rows, gain, shift):
    inv = 1.0 / rows.shape[-1]
    cent = rows - jnp.sum(rows, axis=-1, keepdims=True) * inv
    var = jnp.sum(cent * cent, axis=-1, keepdims=True) * inv
    return cent * lax.rsqrt(var + LN_EPS) * gain + shift


def gelu(x):
    c = 0.7978845608028654
    half = 0.5 * x
    return half + half * jnp.tanh(x * (c + (c * 0.044715) * (x * x)))


def fold(t, op):
    acc = t[0:8]
    for r in range(8, t.shape[0], 8):
        acc = op(acc, t[r:r + 8])
    return acc


def aligned(i, step):
    return pl.ds(pl.multiple_of(i * step, step), step)


def blocks_kernel(cfg, x_hbm, gain_ref, bias_ref, wqkv_hbm, wout_hbm, wup_hbm, wdown_hbm, out_hbm, mid_hbm,
                  wqkv, wout, wup, wdown, xin, xs, a, qkvt, ot, h, nb, nb2, u, y,
                  s0, s1, p0, p1, m0, m1, l0, l1, wsem, xsem, send_sem, own_sem, mid_sem, out_sem):
    n, heads, hd, space_units, time_units = cfg
    units = space_units + time_units
    width = heads * hd
    ff = wup.shape[1]
    tiles = xin.shape[1]
    rows = n * PAIR * SUB
    tok = tiles * rows
    frames = tok // SUB
    groups = rows // SUB
    lanes = width // LANE
    sbuf, pbuf, mbuf, lbuf = (s0, s1), (p0, p1), (m0, m1), (l0, l1)
    cscale = (hd ** -0.5) * LOG2E
    me = lax.axis_index('sp')

    def other(k):
        d = me + k
        return jnp.where(d >= n, d - n, d)

    def xfetch(unit, slot):
        @pl.when(unit < space_units)
        def _():
            for t in range(tiles):
                pltpu.make_async_copy(
                    x_hbm.at[unit, :, pl.ds(t * PAIR, PAIR)], xin.at[slot, t], xsem.at[slot]).start()

        @pl.when(unit >= space_units)
        def _():
            for t in range(tiles):
                pltpu.make_async_copy(
                    mid_hbm.at[:, pl.ds(t * PAIR, PAIR), unit - space_units], xin.at[slot, t], xsem.at[slot]).start()

    def xwait(slot):
        pltpu.make_async_copy(xin.at[slot], xin.at[slot], xsem.at[slot]).wait()

    def mid_wait(t):
        part = mid_hbm.at[pl.ds(0, n - 1), :, pl.ds(t * PAIR, PAIR)]
        pltpu.make_async_copy(part, part, mid_sem.at[t]).wait()

    def wcopy(i, layer):
        src = (wqkv_hbm, wout_hbm, wup_hbm, wdown_hbm)[i]
        return pltpu.make_async_copy(src.at[layer], (wqkv, wout, wup, wdown)[i], wsem.at[i])

    xfetch(0, 0)
    for i in range(4):
        wcopy(i, 0).start()

    barrier = pltpu.get_barrier_semaphore()
    for k in range(1, n):
        pl.semaphore_signal(barrier, inc=1, device_id={'sp': other(k)}, device_id_type=MESH)

    def send(temporal, unit, t, slot):
        if temporal:
            target, sem = out_hbm.at[pl.ds(t * PAIR, PAIR), me * time_units + (unit - space_units)], out_sem
        else:
            target, sem = mid_hbm.at[me, unit, pl.ds(t * PAIR, PAIR)], mid_sem.at[t]
        for k in range(1, n):
            d = other(k)
            pltpu.make_async_remote_copy(
                src_ref=y.at[slot, d], dst_ref=target, send_sem=send_sem.at[slot], recv_sem=sem,
                device_id={'sp': d}, device_id_type=MESH).start()
        pltpu.make_async_copy(y.at[slot, me], target, own_sem.at[slot]).start()

    def own_wait(slot):
        pltpu.make_async_copy(y.at[slot, 0], y.at[slot, 0], own_sem.at[slot]).wait()

    def send_wait(slot):
        whole = y.at[slot, pl.ds(0, n - 1)]
        pltpu.make_async_copy(whole, whole, send_sem.at[slot]).wait()

    gain_all, shift_all = gain_ref[...].astype(F32), bias_ref[...].astype(F32)

    def params(layer, i):
        pick = lambda p: jnp.where(layer > 0, p[2 + i:3 + i], p[i:i + 1])
        return pick(gain_all), pick(shift_all)

    def load_x(slot, t, r0, nr):
        step = PAIR * SUB
        return xin[slot, t, r0 // step:(r0 + nr) // step].reshape(nr, width).astype(F32)

    def pre_norm(temporal, slot, t, r0, nr, par):
        v = normalize(load_x(slot, t, r0, nr), *par)
        if temporal:
            for c in range(lanes):
                xs[c, r0:r0 + nr, :] = v[:, c * LANE:(c + 1) * LANE]
        else:
            a[pl.ds(pl.multiple_of(t * rows + r0, nr), nr), :] = v.astype(BF16)

    def spread(t, g0, ng):
        for p in range(SUB):
            at = pl.ds(pl.multiple_of(p * frames + t * groups + g0, ng), ng)
            for c in range(lanes):
                a[at, c * LANE:(c + 1) * LANE] = xs[c, pl.ds(g0 * SUB + p, ng, stride=SUB), :].astype(BF16)

    def held(c):
        per_buf = tok // LANE
        return sbuf[c // per_buf].at[c % per_buf]

    def mid_norm(temporal, dst, slot, t, r0, nr, par):
        if temporal:
            parts = []
            for g in range(r0 // SUB, (r0 + nr) // SUB):
                at = pl.ds(t * groups + g, SUB, stride=frames)
                parts.append(jnp.concatenate([held(c)[at, :] for c in range(lanes)], axis=1))
            h[t, r0:r0 + nr, :] = (load_x(slot, t, r0, nr) + jnp.concatenate(parts)).astype(BF16)
        dst[r0:r0 + nr, :] = normalize(h[t, r0:r0 + nr, :].astype(F32), *par).astype(BF16)

    nq, nk = tok // QB, tok // KB
    cols = [slice(b * QB, (b + 1) * QB) for b in range(nq)]

    def mix(hh, par, b):
        o = jnp.dot(qkvt[2 * heads + hh], pbuf[par][:, cols[b]], preferred_element_type=F32)
        ot[pl.ds(pl.multiple_of(hh * hd, 8), hd), cols[b]] = o * lbuf[par][:, cols[b]]

    def weigh(par, r0, nr, q, m):
        l = None
        for r in range(r0, r0 + nr, RB):
            e = jnp.exp2((sbuf[par][q // LANE, r:r + RB, :] - m) * cscale)
            pbuf[par][r:r + RB, q:q + LANE] = e.astype(BF16)
            f = fold(e, jnp.add)
            l = f if l is None else l + f
        return l

    def per_lane(b):
        return range(b * QB, (b + 1) * QB, LANE)

    def space_score(hh, par, c):
        k = qkvt[heads + hh, :, c * KB:(c + 1) * KB]
        for b in range(nq):
            s = lax.dot_general(k, qkvt[hh, :, cols[b]], (((0,), (0,)), ((), ())), preferred_element_type=F32)
            for q in per_lane(b):
                sbuf[par][q // LANE, c * KB:(c + 1) * KB, :] = s[:, q - b * QB:q - b * QB + LANE]
            yield fold(s, jnp.maximum)

    def space_first():
        first = None
        for c in range(nk):
            fm = list(space_score(0, 0, c))
            first = fm if first is None else [jnp.maximum(p, q) for p, q in zip(first, fm)]
        for b in range(nq):
            mbuf[0][:, cols[b]] = first[b]

    def space_attend(hs, hm, j):
        ms = [jnp.max(mbuf[j][:, cl], axis=0, keepdims=True) for cl in cols]
        mx = ls = None
        for c in range(nk):
            fm, fl = [], []
            for b, x in enumerate(space_score(hs, 1 - j, c)):
                fm.append(x)
                fl.append(jnp.concatenate(
                    [weigh(j, c * KB, KB, q, ms[b][:, q - b * QB:q - b * QB + LANE]) for q in per_lane(b)], axis=1))
            mx = fm if mx is None else [jnp.maximum(p, q) for p, q in zip(mx, fm)]
            ls = fl if ls is None else [p + q for p, q in zip(ls, fl)]
            if (c + 1) % (nk // nq) == 0:
                mix(hm, 1 - j, (c + 1) // (nk // nq) - 1)
        for b in range(nq):
            mbuf[1 - j][:, cols[b]] = mx[b]
            lbuf[j][:, cols[b]] = 1.0 / jnp.sum(ls[b], axis=0, keepdims=True)

    def span(lo, hi):
        return lo // frames * frames, -(-hi // frames) * frames

    def time_score(hh, par, b):
        kt = jnp.transpose(qkvt[heads + hh])
        lo, hi = span(b * QB, (b + 1) * QB)
        s = jnp.dot(kt[lo:hi], qkvt[hh, :, cols[b]], preferred_element_type=F32)
        for q in per_lane(b):
            mx = None
            k0, k1 = span(q, q + LANE)
            for r in range(k0, k1, frames):
                v = s[r - lo:r - lo + frames, q - b * QB:q - b * QB + LANE]
                lane = q + lax.broadcasted_iota(jnp.int32, v.shape, 1)
                v = jnp.where((lane >= r) & (lane < r + frames), v, NEG)
                sbuf[par][q // LANE, r:r + frames, :] = v
                f = fold(v, jnp.maximum)
                mx = f if mx is None else jnp.maximum(mx, f)
            mbuf[par][:, q:q + LANE] = mx

    def time_soften(par, b):
        for q in per_lane(b):
            k0, k1 = span(q, q + LANE)
            m = jnp.max(mbuf[par][:, q:q + LANE], axis=0, keepdims=True)
            l = weigh(par, k0, k1 - k0, q, m)
            lbuf[par][:, q:q + LANE] = 1.0 / jnp.sum(l, axis=0, keepdims=True)

    def time_first():
        for b in range(nq):
            time_score(0, 0, b)

    def time_attend(hs, hm, j):
        for b in range(nq):
            time_score(hs, 1 - j, b)
            time_soften(j, b)
            mix(hm, 1 - j, b)

    def attention(first, attend, split):
        first()

        def body(i, _):
            def part(j):
                hh = 2 * i + j
                attend(jnp.minimum(hh + 1, heads - 1), jnp.maximum(hh - 1, 0), j)
            part(0)
            if split:
                pl.when(i < heads)(functools.partial(part, 1))
            else:
                part(1)
            return 0
        lax.fori_loop(0, heads // 2, body, 0)

    def unit_body(unit, _):
        slot = lax.rem(unit, 2)
        layer = jnp.where(unit < space_units, 0, 1)
        opening = (unit == 0) | (unit == space_units)
        closing = unit == space_units - 1
        ahead = (unit + 1 < units) & (unit + 1 != space_units)

        def head(temporal):
            xwait(slot)
            par = params(layer, 0)

            def head_norm(t, _):
                pre_norm(temporal, slot, t, 0, rows, par)
                if temporal:
                    spread(t, 0, groups)
                return 0
            lax.fori_loop(0, tiles, head_norm, 0)
            wcopy(0, 0).wait()

        pl.when(unit == 0)(lambda: head(False))

        @pl.when(unit == space_units)
        def _():
            head(True)
            p0[...] = jnp.zeros_like(p0)
            p1[...] = jnp.zeros_like(p1)

        for t in range(1, tiles):
            pl.when(unit + 1 == space_units + t * PAIR)(functools.partial(mid_wait, t))

        @pl.when(ahead)
        def _():
            xfetch(unit + 1, 1 - slot)

        def qkv_body(i, _):
            r = lax.dot_general(wqkv[aligned(i, width), :], a[...], (((1,), (1,)), ((), ())), preferred_element_type=F32)
            qkvt[pl.ds(heads * i, heads)] = r.reshape(heads, hd, tok).astype(BF16)
            return 0
        lax.fori_loop(0, 3, qkv_body, 0)

        @pl.when(closing)
        def _():
            wcopy(0, 1).start()

        pl.when(layer == 0)(lambda: attention(space_first, space_attend, True))
        pl.when(layer == 1)(lambda: attention(time_first, time_attend, False))

        @pl.when(opening)
        def _():
            wcopy(1, 0).wait()

        par1 = params(layer, 1)

        def project(temporal):
            for b in range(nq):
                mix(heads - 1, 1, b)
                r = lax.dot_general(ot[:, cols[b]].astype(BF16), wout[...], (((0,), (0,)), ((), ())),
                                    preferred_element_type=F32)
                if temporal:
                    for c in range(lanes):
                        held(c)[cols[b], :] = r[:, c * LANE:(c + 1) * LANE]
                else:
                    h[b] = (load_x(slot, b, 0, rows) + r).astype(BF16)
                    if b == 0:
                        mid_norm(False, nb, slot, 0, 0, rows, par1)
            if temporal:
                mid_norm(True, nb, slot, 0, 0, rows, par1)

        pl.when(layer == 0)(lambda: project(False))
        pl.when(layer == 1)(lambda: project(True))

        @pl.when(closing)
        def _():
            wcopy(1, 1).start()

        @pl.when(opening)
        def _():
            wcopy(2, 0).wait()
            wcopy(3, 0).wait()

        @pl.when(unit == 0)
        def _():
            pl.semaphore_wait(barrier, n - 1)

        @pl.when(ahead)
        def _():
            xwait(1 - slot)

        par0 = params(layer, 0)
        steps = ff // UPB
        piece = -(-rows // steps // 32) * 32

        def mlp_body(temporal, t, _):
            step = unit * tiles + t
            ys = lax.rem(step, SLOTS)

            @pl.when(step >= SLOTS)
            def _():
                send_wait(ys)

            @pl.when((step >= SLOTS) & ((step < space_units * tiles) | (step >= space_units * tiles + SLOTS)))
            def _():
                own_wait(ys)

            after = jnp.minimum(t + 1, tiles - 1)
            half = rows // 2
            for i in range(steps):
                c = i * UPB
                u[:, c:c + UPB] = gelu(jnp.dot(nb[...], wup[:, c:c + UPB], preferred_element_type=F32)).astype(BF16)
                r0 = i * piece
                if r0 < rows:
                    mid_norm(temporal, nb2, slot, after, r0, piece, par1)
                    pre_norm(temporal, 1 - slot, t, r0, piece, par0)
                    if temporal and (r0 + piece) % half == 0:
                        spread(t, (r0 + piece - half) // SUB, half // SUB)
            cut = ff - UPB
            r = jnp.dot(u[:, :cut], wdown[:cut, :], preferred_element_type=F32)
            r = r + jnp.dot(u[:, cut:], wdown[cut:, :], preferred_element_type=F32)
            y[ys] = (h[t].astype(F32) + r).astype(BF16).reshape(y.shape[1:])
            nb[...] = nb2[...]
            send(temporal, unit, t, ys)
            return 0
        def mlp(temporal):
            lax.fori_loop(0, tiles, functools.partial(mlp_body, temporal), 0)

        for temporal in (False, True):
            pl.when(layer == int(temporal))(functools.partial(mlp, temporal))

        @pl.when(closing)
        def _():
            wcopy(2, 1).start()
            wcopy(3, 1).start()
            for s in range(SLOTS):
                own_wait(s)
            mid_wait(0)
            xfetch(unit + 1, 1 - slot)
        return 0

    lax.fori_loop(0, units, unit_body, 0)
    for s in range(SLOTS):
        send_wait(s)
        own_wait(s)
    got = out_hbm.at[:, pl.ds(0, (n - 1) * time_units)]
    pltpu.make_async_copy(got, got, out_sem).wait()


def run_blocks(n, heads, hd, x, gain, bias, wqkv, wout, wup, wdown):
    local, patches, width = x.shape
    ff = wup.shape[-1]
    per = patches // n // SUB
    x = x.reshape(local, n, per, SUB, width)
    rows = n * PAIR * SUB
    tok = patches
    tiles = tok // rows
    assert tok == n * local * SUB and tiles * PAIR == per == local
    anyspec = pl.BlockSpec(memory_space=pl.ANY)
    vspec = pl.BlockSpec(memory_space=pltpu.VMEM)
    sent = 2 * local * tok * width * 2
    out, _ = pl.pallas_call(
        functools.partial(blocks_kernel, (n, heads, hd, local, per)),
        out_shape=(jax.ShapeDtypeStruct((local, n * per, SUB, width), BF16),
                   jax.ShapeDtypeStruct((n, local, per, SUB, width), BF16)),
        in_specs=[anyspec, vspec, vspec] + [anyspec] * 4,
        out_specs=(anyspec, anyspec),
        scratch_shapes=[
            pltpu.VMEM((3 * width, width), BF16), pltpu.VMEM((width, width), BF16),
            pltpu.VMEM((width, ff), BF16), pltpu.VMEM((ff, width), BF16),
            pltpu.VMEM((2, tiles, n, PAIR, SUB, width), BF16), pltpu.VMEM((width // LANE, rows, LANE), F32),
            pltpu.VMEM((tok, width), BF16), pltpu.VMEM((3 * heads, hd, tok), BF16), pltpu.VMEM((width, tok), F32),
            pltpu.VMEM((tiles, rows, width), BF16), pltpu.VMEM((rows, width), BF16), pltpu.VMEM((rows, width), BF16),
            pltpu.VMEM((rows, ff), BF16), pltpu.VMEM((SLOTS, n, PAIR, SUB, width), BF16),
            pltpu.VMEM((tok // LANE, tok, LANE), F32), pltpu.VMEM((tok // LANE, tok, LANE), F32),
            pltpu.VMEM((tok, tok), BF16), pltpu.VMEM((tok, tok), BF16),
            pltpu.VMEM((8, tok), F32), pltpu.VMEM((8, tok), F32),
            pltpu.VMEM((1, tok), F32), pltpu.VMEM((1, tok), F32),
            pltpu.SemaphoreType.DMA((4,)), pltpu.SemaphoreType.DMA((2,)), pltpu.SemaphoreType.DMA((SLOTS,)),
            pltpu.SemaphoreType.DMA((SLOTS,)), pltpu.SemaphoreType.DMA((tiles,)), pltpu.SemaphoreType.DMA,
        ],
        compiler_params=pltpu.CompilerParams(
            vmem_limit_bytes=67043328, collective_id=0, has_side_effects=True),
        cost_estimate=pl.CostEstimate(flops=48 * local * tok * width * width, bytes_accessed=4 * sent, transcendentals=0),
        name='blocks',
    )(x, gain, bias, wqkv, wout, wup, wdown)
    return out.reshape(local, patches, width)


def solution(mesh):
    act_spec = P('data', 'sp', None, None)
    n = mesh.shape['sp']

    def local_run(x, gain, bias, w_qkv, w_out, w_up, w_down):
        layers, width, _, heads, hd = w_qkv.shape
        wqkvt = jnp.transpose(w_qkv, (0, 2, 3, 4, 1)).reshape(layers, 3 * width, width)
        wo = w_out.reshape(layers, width, width)
        return run_blocks(n, heads, hd, x[0], gain, bias, wqkvt, wo, w_up, w_down)[None]

    return jax.shard_map(local_run, mesh=mesh, in_specs=(act_spec,) + (P(),) * 6, out_specs=act_spec, check_vma=False)
```

```python
import functools

import jax
import jax.numpy as jnp
from jax import lax
from jax.experimental import pallas as pl
from jax.experimental.pallas import tpu as pltpu
from jax.sharding import PartitionSpec as P

F32 = jnp.float32
BF16 = jnp.bfloat16
MESH = pl.DeviceIdType.MESH
LN_EPS = 1e-6
LOG2E = 1.4426950408889634
SUB = 8
PAIR = 2
LANE = 128
QB = 256
KB = 128
RB = 32
UPB = 512
DNB = 512
SLOTS = 3
NEG = -1e38


def normalize(rows, gain, shift):
    inv = 1.0 / rows.shape[-1]
    cent = rows - jnp.sum(rows, axis=-1, keepdims=True) * inv
    var = jnp.sum(cent * cent, axis=-1, keepdims=True) * inv
    return cent * lax.rsqrt(var + LN_EPS) * gain + shift


def gelu(x):
    c = 0.7978845608028654
    half = 0.5 * x
    return half + half * jnp.tanh(x * (c + (c * 0.044715) * (x * x)))


def fold(t, op):
    acc = t[0:8]
    for r in range(8, t.shape[0], 8):
        acc = op(acc, t[r:r + 8])
    return acc


def aligned(i, step):
    return pl.ds(pl.multiple_of(i * step, step), step)


def blocks_kernel(cfg, x_hbm, gain_ref, bias_ref, wqkv_hbm, wout_hbm, wup_hbm, wdown_hbm, out_hbm, mid_hbm,
                  wqkv, wout, wup, wdown, xin, xs, a, qkvt, ot, h, nb, nb2, u, y,
                  s0, s1, p0, p1, m0, m1, l0, l1, qsem, wsem, xsem, send_sem, own_sem, mid_sem, out_sem):
    n, heads, hd, space_units, time_units = cfg
    units = space_units + time_units
    width = heads * hd
    ff = wup.shape[1]
    tiles = xin.shape[1]
    rows = n * PAIR * SUB
    tok = tiles * rows
    frames = tok // SUB
    groups = rows // SUB
    pitch = frames + SUB
    lanes = width // LANE
    sbuf, pbuf, mbuf, lbuf = (s0, s1), (p0, p1), (m0, m1), (l0, l1)
    cscale = (hd ** -0.5) * LOG2E
    me = lax.axis_index('sp')

    def other(k):
        d = me + k
        return jnp.where(d >= n, d - n, d)

    def xfetch(unit, slot):
        @pl.when(unit < space_units)
        def _():
            for t in range(tiles):
                pltpu.make_async_copy(
                    x_hbm.at[unit, :, pl.ds(t * PAIR, PAIR)], xin.at[slot, t], xsem.at[slot]).start()

        @pl.when(unit >= space_units)
        def _():
            for t in range(tiles):
                pltpu.make_async_copy(
                    mid_hbm.at[:, pl.ds(t * PAIR, PAIR), unit - space_units], xin.at[slot, t], xsem.at[slot]).start()

    def xwait(slot):
        pltpu.make_async_copy(xin.at[slot], xin.at[slot], xsem.at[slot]).wait()

    def mid_wait(t):
        part = mid_hbm.at[pl.ds(0, n - 1), :, pl.ds(t * PAIR, PAIR)]
        pltpu.make_async_copy(part, part, mid_sem.at[t]).wait()

    def wcopy(i, layer):
        src = (wout_hbm, wup_hbm, wdown_hbm)[i]
        return pltpu.make_async_copy(src.at[layer], (wout, wup, wdown)[i], wsem.at[i])

    def qkv_copy(i, layer):
        part = aligned(i, width)
        return pltpu.make_async_copy(wqkv_hbm.at[layer, part], wqkv.at[part], qsem.at[i])

    def qkv_fetch(layer):
        for i in range(3):
            qkv_copy(i, layer).start()

    xfetch(0, 0)
    qkv_fetch(0)

    barrier = pltpu.get_barrier_semaphore()
    for k in range(1, n):
        pl.semaphore_signal(barrier, inc=1, device_id={'sp': other(k)}, device_id_type=MESH)

    def send(temporal, unit, t, slot):
        if temporal:
            target, sem = out_hbm.at[pl.ds(t * PAIR, PAIR), me * time_units + (unit - space_units)], out_sem
        else:
            target, sem = mid_hbm.at[me, unit, pl.ds(t * PAIR, PAIR)], mid_sem.at[t]
        for k in range(1, n):
            d = other(k)
            pltpu.make_async_remote_copy(
                src_ref=y.at[slot, d], dst_ref=target, send_sem=send_sem.at[slot], recv_sem=sem,
                device_id={'sp': d}, device_id_type=MESH).start()
        pltpu.make_async_copy(y.at[slot, me], target, own_sem.at[slot]).start()

    def own_wait(slot):
        pltpu.make_async_copy(y.at[slot, 0], y.at[slot, 0], own_sem.at[slot]).wait()

    def send_wait(slot):
        whole = y.at[slot, pl.ds(0, n - 1)]
        pltpu.make_async_copy(whole, whole, send_sem.at[slot]).wait()

    gain_all, shift_all = gain_ref[...].astype(F32), bias_ref[...].astype(F32)

    def params(layer, i):
        pick = lambda p: jnp.where(layer > 0, p[2 + i:3 + i], p[i:i + 1])
        return pick(gain_all), pick(shift_all)

    def load_x(slot, t, r0, nr):
        step = PAIR * SUB
        return xin[slot, t, r0 // step:(r0 + nr) // step].reshape(nr, width).astype(F32)

    def pre_norm(temporal, slot, t, r0, nr, par):
        v = normalize(load_x(slot, t, r0, nr), *par)
        if temporal:
            for c in range(lanes):
                xs[c, r0 % LANE:r0 % LANE + nr, :] = v[:, c * LANE:(c + 1) * LANE]
        else:
            a[pl.ds(pl.multiple_of(t * rows + r0, nr), nr), :] = v.astype(BF16)

    def spread(t, g0, ng):
        for p in range(SUB):
            at = pl.ds(pl.multiple_of(p * frames + t * groups + g0, ng), ng)
            for c in range(lanes):
                a[at, c * LANE:(c + 1) * LANE] = xs[c, pl.ds(p, ng, stride=SUB), :].astype(BF16)

    def held(c):
        per_buf = tok // LANE
        return sbuf[c // per_buf].at[c % per_buf]

    def mid_norm(temporal, dst, slot, t, r0, nr, par):
        if temporal:
            parts = []
            for g in range(r0 // SUB, (r0 + nr) // SUB):
                at = pl.ds(t * groups + g, SUB, stride=pitch)
                parts.append(jnp.concatenate([held(c)[at, :] for c in range(lanes)], axis=1))
            h[t, r0:r0 + nr, :] = (load_x(slot, t, r0, nr) + jnp.concatenate(parts)).astype(BF16)
        dst[r0:r0 + nr, :] = normalize(h[t, r0:r0 + nr, :].astype(F32), *par).astype(BF16)

    nq, nk = tok // QB, tok // KB
    cols = [slice(b * QB, (b + 1) * QB) for b in range(nq)]

    def mix(hh, par, b):
        o = jnp.dot(qkvt[2 * heads + hh], pbuf[par][:, cols[b]], preferred_element_type=F32)
        ot[pl.ds(pl.multiple_of(hh * hd, 8), hd), cols[b]] = o * lbuf[par][:, cols[b]]

    def weigh(par, r0, nr, q, m):
        l = None
        for r in range(r0, r0 + nr, RB):
            e = jnp.exp2((sbuf[par][q // LANE, r:r + RB, :] - m) * cscale)
            pbuf[par][r:r + RB, q:q + LANE] = e.astype(BF16)
            f = fold(e, jnp.add)
            l = f if l is None else l + f
        return l

    def per_lane(b):
        return range(b * QB, (b + 1) * QB, LANE)

    def space_score(hh, par, c):
        k = qkvt[heads + hh, :, c * KB:(c + 1) * KB]
        for b in range(nq):
            s = lax.dot_general(k, qkvt[hh, :, cols[b]], (((0,), (0,)), ((), ())), preferred_element_type=F32)
            for q in per_lane(b):
                sbuf[par][q // LANE, c * KB:(c + 1) * KB, :] = s[:, q - b * QB:q - b * QB + LANE]
            yield fold(s, jnp.maximum)

    def space_first():
        first = None
        for c in range(nk):
            fm = list(space_score(0, 0, c))
            first = fm if first is None else [jnp.maximum(p, q) for p, q in zip(first, fm)]
        for b in range(nq):
            mbuf[0][:, cols[b]] = first[b]

    def space_attend(hs, hm, j):
        ms = [jnp.max(mbuf[j][:, cl], axis=0, keepdims=True) for cl in cols]
        mx = ls = None
        for c in range(nk):
            fm, fl = [], []
            for b, x in enumerate(space_score(hs, 1 - j, c)):
                fm.append(x)
                fl.append(jnp.concatenate(
                    [weigh(j, c * KB, KB, q, ms[b][:, q - b * QB:q - b * QB + LANE]) for q in per_lane(b)], axis=1))
            mx = fm if mx is None else [jnp.maximum(p, q) for p, q in zip(mx, fm)]
            ls = fl if ls is None else [p + q for p, q in zip(ls, fl)]
            if (c + 1) % (nk // nq) == 0:
                mix(hm, 1 - j, (c + 1) // (nk // nq) - 1)
        for b in range(nq):
            mbuf[1 - j][:, cols[b]] = mx[b]
            lbuf[j][:, cols[b]] = 1.0 / jnp.sum(ls[b], axis=0, keepdims=True)

    def span(lo, hi):
        return lo // frames * frames, -(-hi // frames) * frames

    def time_score(hh, par, b):
        kt = jnp.transpose(qkvt[heads + hh])
        lo, hi = span(b * QB, (b + 1) * QB)
        s = jnp.dot(kt[lo:hi], qkvt[hh, :, cols[b]], preferred_element_type=F32)
        for q in per_lane(b):
            mx = None
            k0, k1 = span(q, q + LANE)
            for r in range(k0, k1, frames):
                v = s[r - lo:r - lo + frames, q - b * QB:q - b * QB + LANE]
                lane = q + lax.broadcasted_iota(jnp.int32, v.shape, 1)
                v = jnp.where((lane >= r) & (lane < r + frames), v, NEG)
                sbuf[par][q // LANE, r:r + frames, :] = v
                f = fold(v, jnp.maximum)
                mx = f if mx is None else jnp.maximum(mx, f)
            mbuf[par][:, q:q + LANE] = mx

    def time_soften(par, b):
        for q in per_lane(b):
            k0, k1 = span(q, q + LANE)
            m = jnp.max(mbuf[par][:, q:q + LANE], axis=0, keepdims=True)
            l = weigh(par, k0, k1 - k0, q, m)
            lbuf[par][:, q:q + LANE] = 1.0 / jnp.sum(l, axis=0, keepdims=True)

    def time_first():
        for b in range(nq):
            time_score(0, 0, b)

    def time_attend(hs, hm, j):
        for b in range(nq):
            time_score(hs, 1 - j, b)
            time_soften(j, b)
            mix(hm, 1 - j, b)

    def attention(first, attend, split):
        first()

        def body(i, _):
            def part(j):
                hh = 2 * i + j
                attend(jnp.minimum(hh + 1, heads - 1), jnp.maximum(hh - 1, 0), j)
            part(0)
            if split:
                pl.when(i < heads)(functools.partial(part, 1))
            else:
                part(1)
            return 0
        lax.fori_loop(0, heads // 2, body, 0)

    def unit_body(unit, _):
        slot = lax.rem(unit, 2)
        layer = jnp.where(unit < space_units, 0, 1)
        opening = (unit == 0) | (unit == space_units)
        closing = unit == space_units - 1
        ahead = (unit + 1 < units) & (unit + 1 != space_units)

        def head(temporal):
            xwait(slot)
            par = params(layer, 0)

            def head_norm(t, _):
                for r0 in range(0, rows, LANE):
                    pre_norm(temporal, slot, t, r0, LANE, par)
                    if temporal:
                        spread(t, r0 // SUB, LANE // SUB)
                return 0
            lax.fori_loop(0, tiles, head_norm, 0)
            for i in range(3):
                wcopy(i, layer).start()

        pl.when(unit == 0)(lambda: head(False))

        @pl.when(unit == space_units)
        def _():
            head(True)
            p0[...] = jnp.zeros_like(p0)
            p1[...] = jnp.zeros_like(p1)

        for t in range(1, tiles):
            pl.when(unit + 1 == space_units + t * PAIR)(functools.partial(mid_wait, t))

        @pl.when(ahead)
        def _():
            xfetch(unit + 1, 1 - slot)

        def qkv_body(i, _):
            @pl.when(opening)
            def _():
                qkv_copy(i, 0).wait()
            r = lax.dot_general(wqkv[aligned(i, width), :], a[...], (((1,), (1,)), ((), ())), preferred_element_type=F32)
            qkvt[pl.ds(heads * i, heads)] = r.reshape(heads, hd, tok).astype(BF16)
            return 0
        lax.fori_loop(0, 3, qkv_body, 0)

        @pl.when(closing)
        def _():
            qkv_fetch(1)

        pl.when(layer == 0)(lambda: attention(space_first, space_attend, True))
        pl.when(layer == 1)(lambda: attention(time_first, time_attend, False))

        @pl.when(opening)
        def _():
            wcopy(0, 0).wait()

        par1 = params(layer, 1)

        def project(temporal):
            for b in range(nq):
                mix(heads - 1, 1, b)
                r = lax.dot_general(ot[:, cols[b]].astype(BF16), wout[...], (((0,), (0,)), ((), ())),
                                    preferred_element_type=F32)
                if temporal:
                    lo = b * QB
                    while lo < (b + 1) * QB:
                        p = lo // frames
                        nr = min((p + 1) * frames, (b + 1) * QB) - lo
                        for c in range(lanes):
                            held(c)[lo + p * SUB:lo + p * SUB + nr, :] = r[lo - b * QB:lo - b * QB + nr, c * LANE:(c + 1) * LANE]
                        lo += nr
                else:
                    h[b] = (load_x(slot, b, 0, rows) + r).astype(BF16)
                    if b == 0:
                        mid_norm(False, nb, slot, 0, 0, rows, par1)
            if temporal:
                mid_norm(True, nb, slot, 0, 0, rows, par1)

        pl.when(layer == 0)(lambda: project(False))
        pl.when(layer == 1)(lambda: project(True))

        @pl.when(opening)
        def _():
            wcopy(1, 0).wait()
            wcopy(2, 0).wait()

        @pl.when(unit == 0)
        def _():
            pl.semaphore_wait(barrier, n - 1)

        @pl.when(ahead)
        def _():
            xwait(1 - slot)

        par0 = params(layer, 0)
        steps = ff // UPB
        piece = -(-rows // steps // 32) * 32

        def mlp_body(temporal, t, _):
            step = unit * tiles + t
            ys = lax.rem(step, SLOTS)

            @pl.when(step >= SLOTS)
            def _():
                send_wait(ys)

            @pl.when((step >= SLOTS) & ((step < space_units * tiles) | (step >= space_units * tiles + SLOTS)))
            def _():
                own_wait(ys)

            after = jnp.minimum(t + 1, tiles - 1)

            def now(r0):
                mid_norm(temporal, nb2, slot, after, r0, piece, par1)

            def later(r0):
                pre_norm(temporal, 1 - slot, t, r0, piece, par0)
                if temporal and (r0 + piece) % LANE == 0:
                    spread(t, (r0 + piece - LANE) // SUB, LANE // SUB)

            for i in range(steps):
                c = i * UPB
                u[:, c:c + UPB] = gelu(jnp.dot(nb[...], wup[:, c:c + UPB], preferred_element_type=F32)).astype(BF16)
                if i * piece < rows:
                    now(i * piece)
            cut = ff - 2 * UPB
            left = list(range(0, rows, piece))
            for c in range(0, width, DNB):
                cl = slice(c, min(c + DNB, width))
                r = jnp.dot(u[:, :cut], wdown[:cut, cl], preferred_element_type=F32)
                r = r + jnp.dot(u[:, cut:], wdown[cut:, cl], preferred_element_type=F32)
                y[ys, :, :, :, cl] = (h[t, :, cl].astype(F32) + r).astype(BF16).reshape(y.shape[1:-1] + (-1,))
                for _ in range(-(-rows // piece * DNB // width)):
                    if left:
                        later(left.pop(0))
            while left:
                later(left.pop(0))
            nb[...] = nb2[...]
            send(temporal, unit, t, ys)
            return 0
        def mlp(temporal):
            lax.fori_loop(0, tiles, functools.partial(mlp_body, temporal), 0)

        for temporal in (False, True):
            pl.when(layer == int(temporal))(functools.partial(mlp, temporal))

        @pl.when(closing)
        def _():
            for s in range(SLOTS):
                own_wait(s)
            mid_wait(0)
            xfetch(unit + 1, 1 - slot)
        return 0

    lax.fori_loop(0, units, unit_body, 0)
    for s in range(SLOTS):
        send_wait(s)
        own_wait(s)
    got = out_hbm.at[:, pl.ds(0, (n - 1) * time_units)]
    pltpu.make_async_copy(got, got, out_sem).wait()


def run_blocks(n, heads, hd, x, gain, bias, wqkv, wout, wup, wdown):
    local, patches, width = x.shape
    ff = wup.shape[-1]
    per = patches // n // SUB
    x = x.reshape(local, n, per, SUB, width)
    rows = n * PAIR * SUB
    tok = patches
    tiles = tok // rows
    assert tok == n * local * SUB and tiles * PAIR == per == local
    anyspec = pl.BlockSpec(memory_space=pl.ANY)
    vspec = pl.BlockSpec(memory_space=pltpu.VMEM)
    sent = 2 * local * tok * width * 2
    out, _ = pl.pallas_call(
        functools.partial(blocks_kernel, (n, heads, hd, local, per)),
        out_shape=(jax.ShapeDtypeStruct((local, n * per, SUB, width), BF16),
                   jax.ShapeDtypeStruct((n, local, per, SUB, width), BF16)),
        in_specs=[anyspec, vspec, vspec] + [anyspec] * 4,
        out_specs=(anyspec, anyspec),
        scratch_shapes=[
            pltpu.VMEM((3 * width, width), BF16), pltpu.VMEM((width, width), BF16),
            pltpu.VMEM((width, ff), BF16), pltpu.VMEM((ff, width), BF16),
            pltpu.VMEM((2, tiles, n, PAIR, SUB, width), BF16), pltpu.VMEM((width // LANE, LANE, LANE), F32),
            pltpu.VMEM((tok, width), BF16), pltpu.VMEM((3 * heads, hd, tok), BF16), pltpu.VMEM((width, tok), F32),
            pltpu.VMEM((tiles, rows, width), BF16), pltpu.VMEM((rows, width), BF16), pltpu.VMEM((rows, width), BF16),
            pltpu.VMEM((rows, ff), BF16), pltpu.VMEM((SLOTS, n, PAIR, SUB, width), BF16),
            pltpu.VMEM((tok // LANE, tok + SUB * SUB + SUB, LANE), F32), pltpu.VMEM((tok // LANE, tok + SUB * SUB + SUB, LANE), F32),
            pltpu.VMEM((tok, tok), BF16), pltpu.VMEM((tok, tok), BF16),
            pltpu.VMEM((8, tok), F32), pltpu.VMEM((8, tok), F32),
            pltpu.VMEM((1, tok), F32), pltpu.VMEM((1, tok), F32),
            pltpu.SemaphoreType.DMA((3,)), pltpu.SemaphoreType.DMA((3,)), pltpu.SemaphoreType.DMA((2,)), pltpu.SemaphoreType.DMA((SLOTS,)),
            pltpu.SemaphoreType.DMA((SLOTS,)), pltpu.SemaphoreType.DMA((tiles,)), pltpu.SemaphoreType.DMA,
        ],
        compiler_params=pltpu.CompilerParams(
            vmem_limit_bytes=67043328, collective_id=0, has_side_effects=True),
        cost_estimate=pl.CostEstimate(flops=48 * local * tok * width * width, bytes_accessed=4 * sent, transcendentals=0),
        name='blocks',
    )(x, gain, bias, wqkv, wout, wup, wdown)
    return out.reshape(local, patches, width)


def solution(mesh):
    act_spec = P('data', 'sp', None, None)
    n = mesh.shape['sp']

    def local_run(x, gain, bias, w_qkv, w_out, w_up, w_down):
        layers, width, _, heads, hd = w_qkv.shape
        wqkvt = jnp.transpose(w_qkv, (0, 2, 3, 4, 1)).reshape(layers, 3 * width, width)
        wo = w_out.reshape(layers, width, width)
        return run_blocks(n, heads, hd, x[0], gain, bias, wqkvt, wo, w_up, w_down)[None]

    return jax.shard_map(local_run, mesh=mesh, in_specs=(act_spec,) + (P(),) * 6, out_specs=act_spec, check_vma=False)
```
